32 devices in a mesh: row: 8 (over z, x), col: 4 (over y, core).
Axes of the slice: x: 2, y: 2, z: 4, core: 2. Of those that a mesh axis runs over, the one named last changes fastest.
Arguments:
- panel_block: float32 [20480, 512], P('row', 'col'), may hold values from -12 to 12
- trailing: float32 [20480, 20480], P('row', 'col'), may hold values from -6 to 6
Outputs:
- updated: float32 [20480, 20480], P('row', 'col')
The draws below stay inside these ranges and needn't reach their ends.
All inputs are finite; a program needn't handle non-finite values.
Results may differ from the reference program's by a relative error of at most 0.0003.
Values sent between devices are 32-bit elements; how exact they have to be, the bound alone decides.
A program may use at most 192 MiB of HBM per device.

```python
import math
import jax
import jax.numpy as jnp
from jax import lax

N = 20480
K = 512
N_ROW = 8
N_COL = 4


def draw_panel_block(key, part):
    subkeys = jax.random.split(jax.random.fold_in(key, 11), 3)
    position = jnp.arange(N, dtype=jnp.float32) / N
    rising = 3.0 ** (position - 0.5)
    entries = jax.random.normal(subkeys[0], (N, K), jnp.float32)
    spread = 0.5
    row_scale = 10.0 ** jax.random.uniform(subkeys[1], (N, 1), jnp.float32, -spread, spread)
    col_scale = 10.0 ** jax.random.uniform(subkeys[2], (1, K), jnp.float32, -spread, spread)
    return entries * rising[:, None] * row_scale * col_scale / math.sqrt(K)


def steps_of(stream_key, dims, shards, low, top_value):
    gain, own = 1.0, jax.random.fold_in(stream_key, 6)
    for dim, blocks in shards:
        draws = jnp.exp(jax.random.uniform(jax.random.fold_in(own, dim), (blocks,), jnp.float32, low / len(shards), top_value / len(shards)))
        gain = gain * jnp.repeat(draws, dims[dim] // blocks).reshape([-1 if axis == dim else 1 for axis in range(len(dims))])
    return gain


def centred(own_key, shape, deviation, most, cuts=(), kind=jnp.bfloat16):
    values = deviation * jax.random.normal(own_key, shape, jnp.float32)
    if cuts:
        values = values * steps_of(own_key, shape, cuts, -0.22, 0.18)
    return jnp.clip(values, -most, most).astype(kind)


def setup_inputs(seed: int = 0) -> dict:
    seeds = jax.random.split(jax.random.key(seed), 3)
    panel_block = draw_panel_block(jax.random.fold_in(seeds[2], 71), 0)
    trailing = centred(seeds[1], (N, N), 1.0, 6.0, ((0, 8), (1, 4)), jnp.float32)
    return {"panel_block": panel_block, "trailing": trailing}


def reference(panel_block, trailing):
    local_rows = N // N_ROW
    local_cols = N // N_COL
    squares = jnp.sum(panel_block * panel_block)
    factor = 0.8 * jnp.sqrt(jnp.float32(N)) / jnp.sqrt(squares + 1e-06)
    matrix = panel_block.reshape(N_ROW, local_rows, K).transpose(1, 0, 2).reshape(N, K)
    column_rows = matrix.reshape(local_cols, N_COL, K).transpose(1, 0, 2).reshape(N, K)
    position = jnp.arange(N, dtype=jnp.int32)
    col_index = position % local_cols * N_COL + position // local_cols

    def one_block(pieces):
        row_block, slab_rows, source = pieces
        update = lax.dot_general(row_block, column_rows, (((1,), (1,)), ((), ())), precision=lax.Precision.HIGHEST, preferred_element_type=jnp.float32)
        row_index = jnp.arange(local_rows, dtype=jnp.int32) * N_ROW + source
        lower_part = row_index[:, None] >= col_index[None, :]
        return slab_rows - factor * jnp.where(lower_part, update, jnp.zeros_like(update))
    blocks = lax.map(one_block, (panel_block.reshape(N_ROW, local_rows, K), trailing.reshape(N_ROW, local_rows, N), jnp.arange(N_ROW, dtype=jnp.int32)))
    return blocks.reshape(N, N)
```

```python
import functools

import jax
import jax.numpy as jnp
import numpy as np
from jax import lax
from jax.experimental import pallas as pl
from jax.experimental.pallas import tpu as pltpu
from jax.sharding import PartitionSpec as P

VMEM_LIMIT = 56 * 1024 * 1024


def tile_count(local_rows):
    for count in (5, 4, 2):
        if local_rows % (count * 128) == 0:
            return count
    return 1


def member_table(rows_count, cols_count):
    copies = rows_count // cols_count
    table = np.zeros((cols_count, copies, cols_count), np.int32)
    for c in range(cols_count):
        for h in range(copies):
            for j in range(cols_count):
                if (rows_count, cols_count) == (8, 4):
                    z, y, core = (c // 2) + 2 * h, j // 2, j % 2
                    z_to = z if y == c // 2 else (z + 1) % 4
                    table[c, h, j] = 2 * z_to + core
                else:
                    table[c, h, j] = h * cols_count + j
    return table


def copy_kernel(ti_ref, tj_ref, t_ref, o_ref):
    o_ref[...] = t_ref[...]


def split3(x):
    hi = x.astype(jnp.bfloat16)
    lo = (x - hi.astype(jnp.float32)).astype(jnp.bfloat16)
    return hi, lo


def update_kernel(
    geometry, ti_ref, tj_ref, slot_ref, pos_ref, factor_ref, *refs,
):
    copies, cols_count, rows_count = geometry
    a_refs = refs[:cols_count]
    b_ref, t_ref, prev_ref, o_ref, acat, bcat, mixed = refs[cols_count:]
    step = pl.program_id(0)
    ti, tj = ti_ref[step], tj_ref[step]
    tr, tc = o_ref.shape
    width = b_ref.shape[2]
    depth = cols_count * width

    @pl.when(ti == tj)
    def _():
        for j in range(cols_count):
            for h in range(copies):
                block = b_ref[slot_ref[h * cols_count + j]]
                mixed[pl.ds(h, tr, stride=copies), :] = block
            hi, lo = split3(mixed[...])
            bcat[:, j * width : (j + 1) * width] = hi
            bcat[:, depth + j * width : depth + (j + 1) * width] = lo
            bcat[:, 2 * depth + j * width : 2 * depth + (j + 1) * width] = hi

    for j in range(cols_count):
        hi, lo = split3(a_refs[j][...])
        acat[:, j * width : (j + 1) * width] = hi
        acat[:, depth + j * width : depth + (j + 1) * width] = hi
        acat[:, 2 * depth + j * width : 2 * depth + (j + 1) * width] = lo
    factor = factor_ref[0]
    strips = 4 if tc % 512 == 0 else 1
    sw, sr = tc // strips, tr // strips

    def product(low, s):
        return lax.dot_general(
            acat[low:, :], bcat[s * sw : (s + 1) * sw, :], (((1,), (1,)), ((), ())),
            preferred_element_type=jnp.float32,
        )

    @pl.when(ti != tj)
    def _():
        for s in range(strips):
            cols = slice(s * sw, (s + 1) * sw)
            o_ref[:, cols] = t_ref[:, cols] - factor * product(0, s)

    @pl.when(ti == tj)
    def _():
        for s in range(strips):
            cols = slice(s * sw, (s + 1) * sw)
            low = s * sr
            if low:
                o_ref[:low, cols] = t_ref[:low, cols]
            p = product(low, s)
            row = (lax.broadcasted_iota(jnp.int32, p.shape, 0) + low) * rows_count + pos_ref[0]
            col = (lax.broadcasted_iota(jnp.int32, p.shape, 1) + s * sw) * cols_count + pos_ref[1]
            o_ref[low:, cols] = t_ref[low:, cols] - factor * jnp.where(row >= col, p, 0.0)


def on_device(panel_block, trailing):
    local_rows, width = panel_block.shape
    local_cols = trailing.shape[1]
    rows_count = lax.axis_size("row")
    cols_count = lax.axis_size("col")
    copies = rows_count // cols_count
    total = local_rows * rows_count
    row_owner = lax.axis_index("row")
    col_owner = lax.axis_index("col")
    tiles = tile_count(local_rows)
    tr, tc = local_rows // tiles, local_cols // tiles
    table = member_table(rows_count, cols_count)

    perm = []
    for c in range(cols_count):
        for h in range(copies):
            for j in range(cols_count):
                source = (h * cols_count + c) * cols_count + j
                perm.append((source, int(table[c, h, j]) * cols_count + c))
    moved = lax.ppermute(panel_block, ("row", "col"), perm)
    own, order = [], []
    spread = cols_count // 2
    pairs = [(c, c ^ 1) for c in range(cols_count)]
    for s in range(spread):
        hop = [(c, (c + 2 * s) % cols_count) for c in range(cols_count)]
        straight = lax.ppermute(panel_block, "col", hop) if s else panel_block
        own += [straight, lax.ppermute(straight, "col", pairs)]
        block = (np.arange(cols_count) - 2 * s) % cols_count
        order += [block, block ^ 1]
    order = np.stack(order, axis=1)
    cut = (tiles + 1) // 2
    spans = [(0, cut), (cut, tiles)] if tiles > 1 else [(0, tiles)]
    gathered = []
    for number, (lo, hi) in enumerate(spans):
        piece = moved[lo * tr : hi * tr]
        if number == 0 or rows_count & (rows_count - 1):
            gathered.append((lax.all_gather(piece, "row", axis=0), 0))
            continue
        received = [piece]
        for d in range(1, rows_count):
            partners = [(r, r ^ d) for r in range(rows_count)]
            received.append(lax.ppermute(piece, "row", partners))
        gathered.append((jnp.stack(received), row_owner))
    squares = lax.psum(jnp.sum(panel_block * panel_block), ("row", "col"))
    factor = 0.8 * jnp.sqrt(jnp.float32(total)) / jnp.sqrt(squares + 1e-06)
    factor = factor.reshape(1)
    table = np.stack([table[c][:, order[c]] for c in range(cols_count)])
    slots = jnp.asarray(table.reshape(cols_count, -1))[col_owner]
    pos = jnp.stack([row_owner, col_owner]).astype(jnp.int32)

    shape = jax.ShapeDtypeStruct(trailing.shape, trailing.dtype)
    params = pltpu.CompilerParams(vmem_limit_bytes=VMEM_LIMIT, dimension_semantics=("arbitrary",))
    upper = [(i, j) for j in range(tiles) for i in range(j)]
    if upper:
        ti = jnp.asarray([i for i, _ in upper], jnp.int32)
        tj = jnp.asarray([j for _, j in upper], jnp.int32)
        spec = pl.BlockSpec((tr, tc), lambda s, ti, tj: (ti[s], tj[s]))
        out = pl.pallas_call(
            copy_kernel,
            grid_spec=pltpu.PrefetchScalarGridSpec(
                num_scalar_prefetch=2, grid=(len(upper),), in_specs=[spec], out_specs=spec
            ),
            out_shape=shape,
            compiler_params=params,
            cost_estimate=pl.CostEstimate(
                flops=0, bytes_accessed=len(upper) * tr * tc * 8, transcendentals=0
            ),
            name="upper",
        )(ti, tj, trailing)
    else:
        out = jnp.zeros_like(trailing)

    for (first, last), (part, flip) in zip(spans, gathered):
        todo = [(i, j) for j in range(first, last) for i in range(j, tiles)]
        ti = jnp.asarray([i for i, _ in todo], jnp.int32)
        tj = jnp.asarray([j for _, j in todo], jnp.int32)
        spec = pl.BlockSpec((tr, tc), lambda s, ti, tj, *_: (ti[s], tj[s]))
        out = pl.pallas_call(
            functools.partial(update_kernel, (copies, cols_count, rows_count)),
            grid_spec=pltpu.PrefetchScalarGridSpec(
                num_scalar_prefetch=4,
                grid=(len(todo),),
                in_specs=[
                    pl.BlockSpec(memory_space=pltpu.SMEM),
                    *[pl.BlockSpec((tr, width), lambda s, ti, tj, *_: (ti[s], 0))] * cols_count,
                    pl.BlockSpec(
                        (rows_count, tr, width),
                        lambda s, ti, tj, *_, first=first: (0, tj[s] - first, 0),
                    ),
                    spec,
                    pl.BlockSpec(memory_space=pl.ANY),
                ],
                out_specs=spec,
                scratch_shapes=[
                    pltpu.VMEM((tr, 3 * cols_count * width), jnp.bfloat16),
                    pltpu.VMEM((tc, 3 * cols_count * width), jnp.bfloat16),
                    pltpu.VMEM((tc, width), jnp.float32),
                ],
            ),
            out_shape=shape,
            input_output_aliases={7 + cols_count: 0},
            compiler_params=params,
            cost_estimate=pl.CostEstimate(
                flops=len(todo) * tr * tc * cols_count * width * 6,
                bytes_accessed=len(todo) * tr * tc * 8,
                transcendentals=0,
            ),
            name="update",
        )(ti, tj, slots ^ flip, pos, factor, *own, part, trailing, out)
    return out


def solution(mesh):
    in_specs = (P("row", "col"), P("row", "col"))
    out_specs = P("row", "col")
    return jax.shard_map(
        on_device, mesh=mesh, in_specs=in_specs, out_specs=out_specs, check_vma=False
    )
```
